32 devices in a mesh: group: 4 (over x, core), bl: 8 (over z, y).
Axes of the slice: x: 2, y: 2, z: 4, core: 2. Of those that a mesh axis runs over, the one named last changes fastest.
Arguments:
- visibilities: float32 [2, 512, 16, 1024], P(None, ('group', 'bl')), parts along dimension 1, may hold values from -400 to 400
- flags: int32 [512, 8], P(('group', 'bl')), parts along dimension 0, may hold values 0 or 1
Outputs:
- cross_power: float32 [32, 512, 128], P(None, ('group', 'bl')), parts along dimension 1
- bandpower: float32 [128], P('group'), parts along dimension 0
The draws below stay inside these ranges and needn't reach their ends.
There are 4 independent parts, one for each index of `group`. The reference program is written for one: setup_inputs(seed, part) draws one part's arguments, and reference() takes and returns one part's arrays. A program takes and returns all parts, laid end to end along the dimension named above; each array names one. Nothing has to cross between parts.
All inputs are finite; a program needn't handle non-finite values. No bound on the sum of `flags` on one device may be relied on, other than what follows from the above.
Results may differ from the reference program's by a relative error of at most 0.004.
Values may be sent and summed in bfloat16 or wider, within the bound.
A program may use at most 192 MiB of HBM per device.

```python
import math
import jax
import jax.numpy as jnp
from jax import lax

NF = 1024
NT = 16
CB = 128
BW = 32
BL = 128
NCB = 8


def taper_curve():
    angle = jnp.arange(NF, dtype=jnp.int32).astype(jnp.float32) * (2.0 * math.pi / (NF - 1))
    return 0.35875 - 0.48829 * jnp.cos(angle) + 0.14128 * jnp.cos(2.0 * angle) - 0.01168 * jnp.cos(3.0 * angle)


def draw_visibilities(key, part):
    noise_key = jax.random.fold_in(key, 11)
    shape = (2, BL, NT, NF)
    floor_level = 0.01
    noise = jax.random.truncated_normal(noise_key, -6.0, 6.0, shape, jnp.float32)
    envelope = 0.6 * (1.0 + floor_level) / (taper_curve() + floor_level)
    return (noise * envelope[None, None, None, :]).astype(jnp.float32)


def plant(values, rng, smallest, high):
    extent = values.shape
    place = [jax.random.randint(jax.random.fold_in(rng, axis), (), 0, extent[axis]) for axis in range(len(extent))]
    values = values.at[tuple(place)].set(smallest)
    longest = extent.index(max(extent))
    place[longest] = (place[longest] + 1) % extent[longest]
    return values.at[tuple(place)].set(high)


def setup_inputs(seed: int = 0, part: int = 0) -> dict:
    key_list = jax.random.split(jax.random.key(seed), 3)
    part_keys = jax.random.split(jax.random.fold_in(key_list[2], part), 3)
    visibilities = draw_visibilities(jax.random.fold_in(jax.random.fold_in(key_list[2], part), 71), part)
    flags = plant((jax.random.randint(part_keys[1], (BL, NCB), 0, 8) < 7).astype(jnp.int32), jax.random.fold_in(part_keys[1], 1), 0, 1)
    return dict(visibilities=visibilities, flags=flags)


def make_taper():
    angle = jnp.arange(NF, dtype=jnp.int32).astype(jnp.float32) * (2.0 * math.pi / (NF - 1))
    return 0.35875 - 0.48829 * jnp.cos(angle) + 0.14128 * jnp.cos(2.0 * angle) - 0.01168 * jnp.cos(3.0 * angle)

def make_tables():
    index = jnp.arange(NF, dtype=jnp.int32)
    phase = index[:, None] * index[None, :] % NF
    angle = phase.astype(jnp.float32) * (2.0 * math.pi / NF)
    return (jnp.cos(angle), jnp.sin(angle))

def delay_spectra(visibilities, flags):
    count = visibilities.shape[1]
    keep = jnp.broadcast_to(flags[:, :, None], (count, NF // CB, CB)).reshape(count, NF).astype(jnp.float32)
    weight = keep * make_taper()[None, :]
    tapered = visibilities * weight[None, :, None, :]
    real_rows = tapered[0].reshape(count * NT, NF)
    imag_rows = tapered[1].reshape(count * NT, NF)
    cosine, sine = make_tables()
    high = lax.Precision.HIGHEST
    scale = 1.0 / math.sqrt(NF)
    real_out = (jnp.dot(real_rows, cosine, precision=high) + jnp.dot(imag_rows, sine, precision=high)) * scale
    imag_out = (jnp.dot(imag_rows, cosine, precision=high) - jnp.dot(real_rows, sine, precision=high)) * scale
    stacked = jnp.stack([real_out.reshape(count, NT, NF), imag_out.reshape(count, NT, NF)], 2)
    stacked = stacked.reshape(count, NT, 2, NF // BW, BW).transpose(3, 0, 1, 2, 4)
    return stacked.reshape(NF // BW, count, NT * 2 * BW).astype(jnp.bfloat16)

def reference(visibilities, flags):
    delayed = delay_spectra(visibilities, flags).astype(jnp.float32)
    cross_power = jnp.einsum('kbj,kcj->kbc', delayed, delayed, precision=lax.Precision.HIGHEST) / NT
    self_power = lax.optimization_barrier(jnp.sum(delayed * delayed, axis=2)) / NT
    bandpower = (lax.optimization_barrier(jnp.sum(cross_power, axis=(1, 2))) - lax.optimization_barrier(jnp.sum(self_power, axis=1))) / visibilities.shape[1]
    return (cross_power, bandpower)
```

```python
import functools
import math

import jax
import jax.numpy as jnp
import numpy as np
from jax import lax
from jax.experimental import pallas as pl
from jax.experimental.pallas import tpu as pltpu
from jax.sharding import PartitionSpec as P

BW = 32
LANES = 128
STEPS = 4
MESH = pl.DeviceIdType.MESH
F32 = jnp.float32
BF16 = jnp.bfloat16


def tables(nf, nt):
    radix = nf // LANES
    a = 2.0 * np.pi / (nf - 1) * np.arange(nf)
    taper = 0.35875 - 0.48829 * np.cos(a) + 0.14128 * np.cos(2 * a) - 0.01168 * np.cos(3 * a)
    n = np.arange(LANES)
    angle = 2.0 * np.pi * np.outer(np.arange(radix), n) / nf
    twiddle = np.concatenate([np.cos(angle), -np.sin(angle)], 0)
    phase = 2.0 * np.pi * (np.outer(n, n) % LANES) / LANES
    c, s = np.cos(phase), np.sin(phase)
    scale = 1.0 / math.sqrt(nf * nt)
    table = np.block([[c, -s], [s, c]]) * scale
    per = BW // radix
    table = table.reshape(2 * LANES, 2, 2, LANES // per // 2, per)
    table = table.transpose(0, 2, 3, 1, 4).reshape(2 * LANES, 2 * LANES)
    high = table.astype(np.float32).astype(jnp.bfloat16)
    low = (table - high.astype(np.float64)).astype(np.float32).astype(jnp.bfloat16)
    return (
        taper.reshape(radix, LANES).astype(np.float32),
        twiddle.astype(np.float32),
        high,
        low,
    )


def turn(value, k, size):
    re, im = value
    if k == 0:
        return value
    if 4 * k == size:
        return im, -re
    if 8 * k == size:
        h = math.sqrt(0.5)
        return (re + im) * h, (im - re) * h
    if 8 * k == 3 * size:
        h = math.sqrt(0.5)
        return (im - re) * h, (re + im) * -h
    c, s = math.cos(2 * math.pi * k / size), math.sin(2 * math.pi * k / size)
    return re * c + im * s, im * c - re * s


def short_dft(values):
    size = len(values)
    if size == 1:
        return values
    even, odd = short_dft(values[0::2]), short_dft(values[1::2])
    odd = [turn(v, k, size) for k, v in enumerate(odd)]
    low = [(a + c, b + d) for (a, b), (c, d) in zip(even, odd)]
    high = [(a - c, b - d) for (a, b), (c, d) in zip(even, odd)]
    return low + high


def swap_groups(parts):
    n = len(parts)
    width = LANES // n
    lane = lax.broadcasted_iota(jnp.int32, parts[0].shape, 1)
    bit = 1
    while bit < n:
        upper = (lane // (width * bit)) % 2 == 1
        fresh = list(parts)
        for i in range(n):
            if i & bit:
                continue
            j = i | bit
            fresh[i] = jnp.where(upper, pltpu.roll(parts[j], width * bit, 1), parts[i])
            fresh[j] = jnp.where(upper, parts[j], pltpu.roll(parts[i], LANES - width * bit, 1))
        parts = fresh
        bit *= 2
    return parts


def kernel(
    n, vis, flags_hbm, curves_hbm, table_hbm, home, powers,
    x, flags, curves, table, weight, zhi, zlo, spec, send0, send1, recv0, recv1, back, power,
    in_sem, small_sem, send0_sem, recv0_sem, send1_sem, recv1_sem, own_sem,
    back_sem, home_sem, stay_sem, power_sem, powers_sem, power_stay,
):
    _, count, nt, nf = vis.shape
    radix = nf // LANES
    bands = nf // BW // n
    low = LANES * radix // (2 * BW)
    group = low // radix
    total = n * count
    chunks = nt // STEPS
    piece = STEPS // group * LANES
    half = nt // 2
    me = lax.axis_index("bl")
    order = sorted(range(1, n), key=lambda k: -min(k, n - k))

    barrier = pltpu.get_barrier_semaphore()
    for k in order:
        pl.semaphore_signal(
            barrier, inc=1, device_id={"bl": lax.rem(me + k, n)}, device_id_type=MESH
        )

    def fetch(h, p, q):
        return pltpu.make_async_copy(
            vis.at[p, :, pl.ds(h * half, half), pl.ds(q * LANES, LANES)],
            x.at[p, q, :, pl.ds(h * half, half), :],
            in_sem.at[h, p, q],
        )

    small = [
        pltpu.make_async_copy(source, target, small_sem.at[i])
        for i, (source, target) in enumerate(
            [(flags_hbm, flags), (curves_hbm, curves), (table_hbm, table)]
        )
    ]
    places = [(p, q) for p in range(2) for q in range(radix)]
    for copy in small:
        copy.start()
    for h in range(2):
        for p, q in places:
            fetch(h, p, q).start()

    for copy in small:
        copy.wait()
    diagonal = lax.broadcasted_iota(jnp.int32, (count, count), 0) == lax.broadcasted_iota(
        jnp.int32, (count, count), 1
    )
    for q in range(radix):
        keep = jnp.where(diagonal, flags[q : q + 1, :].astype(F32), 0.0)
        weight[q] = jnp.sum(keep, axis=1, keepdims=True) * curves[q : q + 1, :]

    rows_view = x.reshape(2 * radix * count * nt, LANES)

    def produce(t0, store):
        for s in range(STEPS):
            t = t0 + s
            values = []
            for q in range(radix):
                pair = [
                    rows_view[pl.ds((p * radix + q) * count * nt + t, count, stride=nt), :]
                    * weight[q]
                    for p in range(2)
                ]
                values.append(tuple(pair))
            for r, (re, im) in enumerate(short_dft(values)):
                if r:
                    c_r = curves[radix + r : radix + r + 1, :]
                    s_r = curves[2 * radix + r : 2 * radix + r + 1, :]
                    re, im = re * c_r - im * s_r, re * s_r + im * c_r
                z = jnp.concatenate([re, im], 1)
                z_hi = z.astype(BF16)
                at = pl.ds((s * radix + r) * count, count)
                zhi[at, :] = z_hi
                zlo[at, :] = (z - z_hi.astype(F32)).astype(BF16)
        dot = functools.partial(jnp.dot, preferred_element_type=F32)
        spec[...] = (
            dot(zhi[...], table[0]) + dot(zlo[...], table[0]) + dot(zhi[...], table[1])
        )
        for g in range(STEPS // group):
            for h in range(2):
                blocks = [
                    spec[pl.ds(((g * group + s) * radix + r) * count, count), pl.ds(h * LANES, LANES)]
                    for s in range(group)
                    for r in range(radix)
                ]
                for b, block in enumerate(swap_groups(blocks)):
                    store(h * low + b, g, block.astype(BF16))

    def forward0(peer, slot):
        return pltpu.make_async_remote_copy(
            src_ref=send0.at[peer],
            dst_ref=recv0.at[slot],
            send_sem=send0_sem.at[peer],
            recv_sem=recv0_sem.at[slot],
            device_id={"bl": peer},
            device_id_type=MESH,
        )

    def forward1(kb, peer, slot):
        return pltpu.make_async_remote_copy(
            src_ref=send1.at[peer, kb],
            dst_ref=recv1.at[slot, kb],
            send_sem=send1_sem.at[kb, peer],
            recv_sem=recv1_sem.at[kb, slot],
            device_id={"bl": peer},
            device_id_type=MESH,
        )

    own0 = pltpu.make_async_copy(send0.at[me], recv0.at[me], own_sem.at[0])
    own1 = pltpu.make_async_copy(send1.at[me], recv1.at[me], own_sem.at[1])

    for p, q in places:
        fetch(0, p, q).wait()

    def store0(band, g, block):
        send0[band // bands, band % bands, :, g * LANES : (g + 1) * LANES] = block

    produce(0, store0)
    pl.semaphore_wait(barrier, n - 1)
    for k in order:
        forward0(lax.rem(me + k, n), me).start()
    own0.start()

    for h in range(2):
        if h:
            for p, q in places:
                fetch(1, p, q).wait()

        @pl.loop(max(1, h * chunks // 2), (h + 1) * chunks // 2)
        def _(c):
            def store1(band, g, block):
                at = pl.ds(pl.multiple_of((c - 1) * piece + g * LANES, LANES), LANES)
                send1[band // bands, band % bands, :, at] = block

            produce(c * STEPS, store1)

    for kb in range(bands):
        for k in order:
            forward1(kb, lax.rem(me + k, n), me).start()
    own1.start()

    def homeward(kb, peer, slot):
        return pltpu.make_async_remote_copy(
            src_ref=back.at[kb, peer],
            dst_ref=home.at[slot, kb],
            send_sem=back_sem.at[kb, peer],
            recv_sem=home_sem.at[kb, slot],
            device_id={"bl": peer},
            device_id_type=MESH,
        )

    def stay(kb):
        return pltpu.make_async_copy(back.at[kb, me], home.at[me, kb], stay_sem.at[kb])

    def spread(peer, slot):
        return pltpu.make_async_remote_copy(
            src_ref=power,
            dst_ref=powers.at[slot],
            send_sem=power_sem.at[peer],
            recv_sem=powers_sem.at[slot],
            device_id={"bl": peer},
            device_id_type=MESH,
        )

    own0.wait()
    for k in reversed(order):
        peer = lax.rem(me + k, n)
        forward0(peer, peer).wait_recv()
    own1.wait()

    row = lax.broadcasted_iota(jnp.int32, (total, total), 0)
    col = lax.broadcasted_iota(jnp.int32, (total, total), 1)
    spot = lax.broadcasted_iota(jnp.int32, (1, LANES), 1)
    extra = jnp.zeros((1, LANES), F32)
    gram = functools.partial(
        lax.dot_general,
        dimension_numbers=(((1,), (1,)), ((), ())),
        preferred_element_type=F32,
    )
    for kb in range(bands):
        for k in reversed(order):
            peer = lax.rem(me + k, n)
            forward1(kb, peer, peer).wait_recv()
        first = recv0[:, kb].reshape(total, recv0.shape[3])
        rest = recv1[:, kb].reshape(total, recv1.shape[3])
        cross = gram(first, first) + gram(rest, rest)
        back[kb] = cross.astype(BF16).reshape(n, count, total)
        for k in order:
            homeward(kb, lax.rem(me + k, n), me).start()
        stay(kb).start()
        side = jnp.sum(jnp.where(row != col, cross, 0.0), axis=0, keepdims=True)
        side = jnp.sum(side, axis=1, keepdims=True) * (1.0 / total)
        extra += jnp.where(spot == me * bands + kb, side, 0.0)
    power[...] = extra
    for k in order:
        spread(lax.rem(me + k, n), me).start()
    last = pltpu.make_async_copy(power, powers.at[me], power_stay)
    last.start()

    for k in order:
        peer = lax.rem(me + k, n)
        forward0(peer, me).wait_send()
        for kb in range(bands):
            forward1(kb, peer, me).wait_send()
    for kb in range(bands):
        stay(kb).wait()
    last.wait()
    for kb in range(bands):
        for k in reversed(order):
            peer = lax.rem(me + k, n)
            homeward(kb, peer, peer).wait_recv()
    for k in reversed(order):
        peer = lax.rem(me + k, n)
        spread(peer, peer).wait_recv()
    for k in order:
        peer = lax.rem(me + k, n)
        for kb in range(bands):
            homeward(kb, peer, me).wait_send()
        spread(peer, me).wait_send()


def unpack(home, powers, cross, band):
    n, bands = home.shape[:2]
    for d in range(n):
        for kb in range(bands):
            cross[d * bands + kb] = home[d, kb].astype(F32)
    band[...] = jnp.sum(powers[...], axis=0)[:, : n * bands]


def shards(n, visibilities, flags):
    _, count, nt, nf = visibilities.shape
    radix = nf // LANES
    total = n * count
    bands = nf // BW // n
    taper, twiddle, high, low = tables(nf, nt)
    curves = jnp.asarray(np.concatenate([taper, twiddle], 0))
    table = jnp.asarray(np.stack([high, low]))
    turned = flags.T
    rows = STEPS * radix * count
    near, far = STEPS * 2 * BW, (nt - STEPS) * 2 * BW
    vmem = pl.BlockSpec(memory_space=pltpu.VMEM)
    dma = pltpu.SemaphoreType.DMA
    home, powers = pl.pallas_call(
        functools.partial(kernel, n),
        out_shape=[
            pltpu.VMEM((n, bands, count, total), BF16),
            pltpu.VMEM((n, 1, LANES), F32),
        ],
        in_specs=[pl.BlockSpec(memory_space=pltpu.HBM)] * 4,
        out_specs=[vmem, vmem],
        scratch_shapes=[
            pltpu.VMEM((2, radix, count, nt, LANES), F32),
            pltpu.VMEM(turned.shape, turned.dtype),
            pltpu.VMEM(curves.shape, curves.dtype),
            pltpu.VMEM(table.shape, table.dtype),
            pltpu.VMEM((radix, count, LANES), F32),
            pltpu.VMEM((rows, 2 * LANES), BF16),
            pltpu.VMEM((rows, 2 * LANES), BF16),
            pltpu.VMEM((rows, 2 * LANES), F32),
            pltpu.VMEM((n, bands, count, near), BF16),
            pltpu.VMEM((n, bands, count, far), BF16),
            pltpu.VMEM((n, bands, count, near), BF16),
            pltpu.VMEM((n, bands, count, far), BF16),
            pltpu.VMEM((bands, n, count, total), BF16),
            pltpu.VMEM((1, LANES), F32),
            dma((2, 2, radix)),
            dma((3,)),
            dma((n,)),
            dma((n,)),
            dma((bands, n)),
            dma((bands, n)),
            dma((2,)),
            dma((bands, n)),
            dma((bands, n)),
            dma((bands,)),
            dma((n,)),
            dma((n,)),
            dma,
        ],
        compiler_params=pltpu.CompilerParams(
            collective_id=0, has_side_effects=True, vmem_limit_bytes=60 * 1024 * 1024
        ),
    )(visibilities, turned, curves, table)
    cross, band = pl.pallas_call(
        unpack,
        out_shape=[
            jax.ShapeDtypeStruct((nf // BW, count, total), F32),
            jax.ShapeDtypeStruct((1, nf // BW), F32),
        ],
        in_specs=[vmem, vmem],
        out_specs=[vmem, vmem],
        compiler_params=pltpu.CompilerParams(vmem_limit_bytes=8 * 1024 * 1024),
    )(home, powers)
    return cross, band.reshape(nf // BW)


def solution(mesh):
    return jax.shard_map(
        functools.partial(shards, mesh.shape["bl"]),
        mesh=mesh,
        in_specs=(P(None, ("group", "bl"), None, None), P(("group", "bl"), None)),
        out_specs=(P(None, ("group", "bl"), None), P("group")),
        check_vma=False,
    )
```

```python
import functools
import math

import jax
import jax.numpy as jnp
import numpy as np
from jax import lax
from jax.experimental import pallas as pl
from jax.experimental.pallas import tpu as pltpu
from jax.sharding import PartitionSpec as P

BW = 32
LANES = 128
STEPS = 4
MESH = pl.DeviceIdType.MESH
F32 = jnp.float32
BF16 = jnp.bfloat16


def tables(nf, nt):
    radix = nf // LANES
    a = 2.0 * np.pi / (nf - 1) * np.arange(nf)
    taper = 0.35875 - 0.48829 * np.cos(a) + 0.14128 * np.cos(2 * a) - 0.01168 * np.cos(3 * a)
    n = np.arange(LANES)
    angle = 2.0 * np.pi * np.outer(np.arange(radix), n) / nf
    twiddle = np.concatenate([np.cos(angle), -np.sin(angle)], 0)
    phase = 2.0 * np.pi * (np.outer(n, n) % LANES) / LANES
    c, s = np.cos(phase), np.sin(phase)
    scale = 1.0 / math.sqrt(nf * nt)
    table = np.block([[c, -s], [s, c]]) * scale
    per = BW // radix
    table = table.reshape(2 * LANES, 2, 2, LANES // per // 2, per)
    table = table.transpose(0, 2, 3, 1, 4).reshape(2 * LANES, 2 * LANES)
    high = table.astype(np.float32).astype(jnp.bfloat16)
    low = (table - high.astype(np.float64)).astype(np.float32).astype(jnp.bfloat16)
    return (
        taper.reshape(radix, LANES).astype(np.float32),
        twiddle.astype(np.float32),
        high,
        low,
    )


def turn(value, k, size):
    re, im = value
    if k == 0:
        return value
    if 4 * k == size:
        return im, -re
    if 8 * k == size:
        h = math.sqrt(0.5)
        return (re + im) * h, (im - re) * h
    if 8 * k == 3 * size:
        h = math.sqrt(0.5)
        return (im - re) * h, (re + im) * -h
    c, s = math.cos(2 * math.pi * k / size), math.sin(2 * math.pi * k / size)
    return re * c + im * s, im * c - re * s


def short_dft(values):
    size = len(values)
    if size == 1:
        return values
    even, odd = short_dft(values[0::2]), short_dft(values[1::2])
    odd = [turn(v, k, size) for k, v in enumerate(odd)]
    low = [(a + c, b + d) for (a, b), (c, d) in zip(even, odd)]
    high = [(a - c, b - d) for (a, b), (c, d) in zip(even, odd)]
    return low + high


def swap_groups(parts):
    n = len(parts)
    width = LANES // n
    lane = lax.broadcasted_iota(jnp.int32, parts[0].shape, 1)
    bit = 1
    while bit < n:
        upper = (lane // (width * bit)) % 2 == 1
        fresh = list(parts)
        for i in range(n):
            if i & bit:
                continue
            j = i | bit
            fresh[i] = jnp.where(upper, pltpu.roll(parts[j], width * bit, 1), parts[i])
            fresh[j] = jnp.where(upper, parts[j], pltpu.roll(parts[i], LANES - width * bit, 1))
        parts = fresh
        bit *= 2
    return parts


def kernel(
    n, vis, flags_hbm, curves_hbm, table_hbm, home, powers,
    x, flags, curves, table, weight, zhi, zlo, spec, send0, send1, recv0, recv1, back, power,
    in_sem, small_sem, send_sem, recv0_sem, recv1_sem, home_sem,
):
    _, count, nt, nf = vis.shape
    radix = nf // LANES
    bands = nf // BW // n
    low = LANES * radix // (2 * BW)
    group = low // radix
    total = n * count
    chunks = nt // STEPS
    piece = STEPS // group * LANES
    half = nt // 2
    me = lax.axis_index("bl")
    late = [k for k in range(1, n) if k >= 3 * n // 4]
    order = [k for k in range(1, n) if k not in late] + late

    barrier = pltpu.get_barrier_semaphore()
    for k in order:
        pl.semaphore_signal(barrier, inc=1, device_id={"bl": me ^ k}, device_id_type=MESH)

    def await_bytes(ref, sem):
        pltpu.make_async_copy(ref, ref, sem).wait()

    small = [
        pltpu.make_async_copy(source, target, small_sem.at[i])
        for i, (source, target) in enumerate(
            [(flags_hbm, flags), (curves_hbm, curves), (table_hbm, table)]
        )
    ]
    for copy in small:
        copy.start()
    for h in range(2):
        for p in range(2):
            for q in range(radix):
                pltpu.make_async_copy(
                    vis.at[p, :, pl.ds(h * half, half), pl.ds(q * LANES, LANES)],
                    x.at[h, p, q],
                    in_sem.at[h],
                ).start()

    for copy in small:
        copy.wait()
    diagonal = lax.broadcasted_iota(jnp.int32, (count, count), 0) == lax.broadcasted_iota(
        jnp.int32, (count, count), 1
    )
    for q in range(radix):
        keep = jnp.where(diagonal, flags[q : q + 1, :].astype(F32), 0.0)
        weight[q] = jnp.sum(keep, axis=1, keepdims=True) * curves[q : q + 1, :]

    rows_view = x.reshape(2 * 2 * radix * count * half, LANES)

    def produce(h, t0, store):
        for s in range(STEPS):
            t = t0 + s
            values = []
            for q in range(radix):
                pair = [
                    rows_view[
                        pl.ds(((h * 2 + p) * radix + q) * count * half + t, count, stride=half), :
                    ]
                    * weight[q]
                    for p in range(2)
                ]
                values.append(tuple(pair))
            for r, (re, im) in enumerate(short_dft(values)):
                if r:
                    c_r = curves[radix + r : radix + r + 1, :]
                    s_r = curves[2 * radix + r : 2 * radix + r + 1, :]
                    re, im = re * c_r - im * s_r, re * s_r + im * c_r
                z = jnp.concatenate([re, im], 1)
                z_hi = z.astype(BF16)
                at = pl.ds((s * radix + r) * count, count)
                zhi[at, :] = z_hi
                zlo[at, :] = (z - z_hi.astype(F32)).astype(BF16)
        dot = functools.partial(jnp.dot, preferred_element_type=F32)
        spec[...] = (
            dot(zhi[...], table[0]) + dot(zlo[...], table[0]) + dot(zhi[...], table[1])
        )
        for g in range(STEPS // group):
            for p in range(2):
                blocks = [
                    spec[pl.ds(((g * group + s) * radix + r) * count, count), pl.ds(p * LANES, LANES)]
                    for s in range(group)
                    for r in range(radix)
                ]
                for b, block in enumerate(swap_groups(blocks)):
                    store(p * low + b, g, block.astype(BF16))

    def remote(source, target, send, recv, peer):
        return pltpu.make_async_remote_copy(
            src_ref=source,
            dst_ref=target,
            send_sem=send_sem.at[send],
            recv_sem=recv,
            device_id={"bl": peer},
            device_id_type=MESH,
        )

    await_bytes(x.at[0], in_sem.at[0])

    def store0(band, g, block):
        send0[band // bands, band % bands, :, g * LANES : (g + 1) * LANES] = block

    produce(0, 0, store0)
    pl.semaphore_wait(barrier, n - 1)
    for k in order:
        remote(send0.at[me ^ k], recv0.at[me], 0, recv0_sem, me ^ k).start()
    pltpu.make_async_copy(send0.at[me], recv0.at[me], recv0_sem).start()

    for h in range(2):
        if h:
            await_bytes(x.at[1], in_sem.at[1])
        first = 0 if h else 1

        @pl.loop(first, chunks // 2)
        def _(c):
            def store1(band, g, block):
                start = (h * (chunks // 2) + c - 1) * piece + g * LANES
                at = pl.ds(pl.multiple_of(start, LANES), LANES)
                send1[band // bands, band % bands, :, at] = block

            produce(h, c * STEPS, store1)

    def forward(kb, peer):
        remote(send1.at[peer, kb], recv1.at[me, kb], 1, recv1_sem.at[kb], peer).start()

    for k in order:
        if k not in late:
            for kb in range(bands):
                forward(kb, me ^ k)
    for kb in range(bands):
        for k in late:
            forward(kb, me ^ k)
    for kb in range(bands):
        pltpu.make_async_copy(send1.at[me, kb], recv1.at[me, kb], recv1_sem.at[kb]).start()

    row = lax.broadcasted_iota(jnp.int32, (total, total), 0)
    col = lax.broadcasted_iota(jnp.int32, (total, total), 1)
    spot = lax.broadcasted_iota(jnp.int32, (1, LANES), 1)
    extra = jnp.zeros((1, LANES), F32)
    gram = functools.partial(
        lax.dot_general,
        dimension_numbers=(((1,), (1,)), ((), ())),
        preferred_element_type=F32,
    )
    await_bytes(recv0, recv0_sem)
    for kb in range(bands):
        await_bytes(recv1.at[:, kb], recv1_sem.at[kb])
        first = recv0[:, kb].reshape(total, recv0.shape[3])
        rest = recv1[:, kb].reshape(total, recv1.shape[3])
        cross = gram(first, first) + gram(rest, rest)
        back[:, kb] = cross.astype(BF16).reshape(n, count, total)
        for k in order:
            remote(back.at[me ^ k, kb], home.at[me, kb], 2, home_sem.at[0], me ^ k).start()
        pltpu.make_async_copy(back.at[me, kb], home.at[me, kb], home_sem.at[0]).start()
        side = jnp.sum(jnp.where(row != col, cross, 0.0), axis=0, keepdims=True)
        side = jnp.sum(side, axis=1, keepdims=True) * (1.0 / total)
        extra += jnp.where(spot == me * bands + kb, side, 0.0)
    power[...] = extra
    for k in order:
        remote(power, powers.at[me], 3, home_sem.at[1], me ^ k).start()
    pltpu.make_async_copy(power, powers.at[me], home_sem.at[1]).start()

    others = pl.ds(0, n - 1)
    await_bytes(send0.at[others], send_sem.at[0])
    await_bytes(send1.at[others], send_sem.at[1])
    await_bytes(back.at[others], send_sem.at[2])
    await_bytes(powers.at[others], send_sem.at[3])
    await_bytes(home, home_sem.at[0])
    await_bytes(powers, home_sem.at[1])


def unpack(home, powers, cross, band):
    n, bands = home.shape[:2]
    for d in range(n):
        for kb in range(bands):
            cross[d * bands + kb] = home[d, kb].astype(F32)
    band[...] = jnp.sum(powers[...], axis=0)[:, : n * bands]


def shards(n, visibilities, flags):
    _, count, nt, nf = visibilities.shape
    radix = nf // LANES
    total = n * count
    bands = nf // BW // n
    taper, twiddle, high, low = tables(nf, nt)
    curves = jnp.asarray(np.concatenate([taper, twiddle], 0))
    table = jnp.asarray(np.stack([high, low]))
    turned = flags.T
    rows = STEPS * radix * count
    near, far = STEPS * 2 * BW, (nt - STEPS) * 2 * BW
    vmem = pl.BlockSpec(memory_space=pltpu.VMEM)
    dma = pltpu.SemaphoreType.DMA
    home, powers = pl.pallas_call(
        functools.partial(kernel, n),
        out_shape=[
            pltpu.VMEM((n, bands, count, total), BF16),
            pltpu.VMEM((n, 1, LANES), F32),
        ],
        in_specs=[pl.BlockSpec(memory_space=pltpu.HBM)] * 4,
        out_specs=[vmem, vmem],
        scratch_shapes=[
            pltpu.VMEM((2, 2, radix, count, nt // 2, LANES), F32),
            pltpu.VMEM(turned.shape, turned.dtype),
            pltpu.VMEM(curves.shape, curves.dtype),
            pltpu.VMEM(table.shape, table.dtype),
            pltpu.VMEM((radix, count, LANES), F32),
            pltpu.VMEM((rows, 2 * LANES), BF16),
            pltpu.VMEM((rows, 2 * LANES), BF16),
            pltpu.VMEM((rows, 2 * LANES), F32),
            pltpu.VMEM((n, bands, count, near), BF16),
            pltpu.VMEM((n, bands, count, far), BF16),
            pltpu.VMEM((n, bands, count, near), BF16),
            pltpu.VMEM((n, bands, count, far), BF16),
            pltpu.VMEM((n, bands, count, total), BF16),
            pltpu.VMEM((1, LANES), F32),
            dma((2,)),
            dma((3,)),
            dma((4,)),
            dma,
            dma((bands,)),
            dma((2,)),
        ],
        compiler_params=pltpu.CompilerParams(
            collective_id=0, has_side_effects=True, vmem_limit_bytes=60 * 1024 * 1024
        ),
    )(visibilities, turned, curves, table)
    cross, band = pl.pallas_call(
        unpack,
        out_shape=[
            jax.ShapeDtypeStruct((nf // BW, count, total), F32),
            jax.ShapeDtypeStruct((1, nf // BW), F32),
        ],
        in_specs=[vmem, vmem],
        out_specs=[vmem, vmem],
        compiler_params=pltpu.CompilerParams(vmem_limit_bytes=8 * 1024 * 1024),
    )(home, powers)
    return cross, band.reshape(nf // BW)


def solution(mesh):
    return jax.shard_map(
        functools.partial(shards, mesh.shape["bl"]),
        mesh=mesh,
        in_specs=(P(None, ("group", "bl"), None, None), P(("group", "bl"), None)),
        out_specs=(P(None, ("group", "bl"), None), P("group")),
        check_vma=False,
    )
```
